32 devices in a mesh: enc: 8 (over z, x), dec: 2 (over y), grp: 2 (over core).
Axes of the slice: x: 2, y: 2, z: 4, core: 2. Of those that a mesh axis runs over, the one named last changes fastest.
Arguments:
- images: bfloat16 [32, 4, 32, 1280], P(('enc', 'dec', 'grp')), may hold values from -6 to 6
- ln_gain: float32 [1280], replicated, may hold values from 0.1 to 1.9
- ln_bias: float32 [1280], replicated, may hold values from -3 to 3
- fc1_weight: bfloat16 [5120, 1280], P('enc'), may hold values from -0.15625 to 0.15625
- fc1_bias: float32 [5120], P('enc'), may hold values from -3 to 3
- fc2_weight: bfloat16 [5120, 1280], P('enc'), may hold values from -0.078125 to 0.078125
- fc2_bias: float32 [1280], replicated, may hold values from -3 to 3
- key_weight: bfloat16 [1280, 512], replicated, may hold values from -0.15625 to 0.15625
- value_weight: bfloat16 [1280, 512], replicated, may hold values from -0.15625 to 0.15625
- text: bfloat16 [32, 128, 8192], P(('enc', 'grp')), may hold values from -6 to 6
- query_weight: bfloat16 [8192, 4096], P('enc', 'dec'), may hold values from -0.0625 to 0.0625
- tiles: int32 [8, 2, 2], replicated, may hold values from 1 to 4, as said below
- links: int32 [32, 2], P(('enc', 'grp')), may hold values from 0 to 1, as said below
- lengths: int32 [32], P(('enc', 'grp')), may hold values from 1 to 128
- state_grads: bfloat16 [32, 4, 32, 1280], P(('enc', 'dec', 'grp')), may hold values from -0.125 to 0.125
Outputs:
- context: bfloat16 [32, 128, 4096], P(('enc', 'grp'), None, 'dec')
- fc1_grad: float32 [5120, 1280], P(('enc', 'dec', 'grp'))
- fc2_grad: float32 [5120, 1280], P(('enc', 'dec', 'grp'))
The draws below stay inside these ranges and needn't reach their ends.
Inputs may be any that keep to these rules, and one draw needn't show every extreme that they name: The 8 images that share their last two indices have 20 tiles together, and one of them has 4. `links`: every text is linked to at least one image.
All inputs are finite; a program needn't handle non-finite values.
Results may differ from the reference program's by a relative error of at most 0.017.
Values may be sent and summed in bfloat16 or wider, within the bound.
A program may use at most 128 MiB of HBM per device.

```python
import jax
import jax.numpy as jnp
from jax import lax

DV = 1280
FF = 5120
DT = 8192
HEADS = 32
KV_HEADS = 4
HD = 128
TXT = 128
TILES = 4
PATCH = 32
SAMP = 2
IMAGES = 32
TEXTS = 32
N_ENC = 8
N_DEC = 2
N_GRP = 2


def draw_tiles(key, part):
    groups = N_DEC * N_GRP
    group_keys = jax.random.split(jax.random.fold_in(key, 11), groups)

    def one_group(group_key):
        first_key, second_key = jax.random.split(group_key)
        shuffled = jax.random.permutation(first_key, 3 * (N_ENC - 1))
        chosen = (shuffled < 3 * N_ENC // 2 - 3).astype(jnp.int32)
        others = jnp.sum(chosen.reshape(N_ENC - 1, 3), axis=1)
        forced = jax.random.randint(second_key, (), 0, N_ENC)
        index = jnp.arange(N_ENC)
        earlier = jnp.take(others, jnp.clip(index, 0, N_ENC - 2))
        later = jnp.take(others, jnp.clip(index - 1, 0, N_ENC - 2))
        extra = jnp.where(index < forced, earlier, jnp.where(index == forced, 3, later))
        return 1 + extra
    columns = jax.vmap(one_group)(group_keys)
    return columns.T.reshape(N_ENC, N_DEC, N_GRP).astype(jnp.int32)


def draw_links(key, part):
    first_key, second_key = jax.random.split(jax.random.fold_in(key, 23))
    coins = jax.random.randint(first_key, (TEXTS, N_DEC), 0, 5)
    chosen = jax.random.randint(second_key, (TEXTS, 1), 0, N_DEC)
    column = jnp.arange(N_DEC)[None, :]
    return jnp.where((coins < 2) | (column == chosen), 1, 0).astype(jnp.int32)


def with_ends(array, rng, least, high):
    extent = array.shape
    index_at = [jax.random.randint(jax.random.fold_in(rng, axis), (), 0, extent[axis]) for axis in range(len(extent))]
    array = array.at[tuple(index_at)].set(least)
    longest = extent.index(max(extent))
    index_at[longest] = (index_at[longest] + 1) % extent[longest]
    return array.at[tuple(index_at)].set(high)


def steps_of(rng, extent, shards, smallest, largest):
    def one(position, shards_of):
        draws = jax.random.uniform(jax.random.fold_in(jax.random.fold_in(rng, 6), position), (shards_of,), jnp.float32, smallest / len(shards), largest / len(shards))
        return jnp.repeat(jnp.exp(draws), extent[position] // shards_of).reshape((-1,) + (1,) * (len(extent) - position - 1))

    level = one(*shards[0])
    for cut in shards[1:]:
        level = level * one(*cut)
    return level


def normal_values(own_key, shape, scale, bound, cuts=(), kind=jnp.bfloat16):
    entries = scale * jax.random.normal(own_key, shape, jnp.float32)
    if cuts:
        entries = entries * steps_of(own_key, shape, cuts, -0.22, 0.18)
    return jnp.clip(entries, -bound, bound).astype(kind)


def setup_inputs(seed: int = 0) -> dict:
    streams_of = jax.random.split(jax.random.key(seed), 16)
    images = normal_values(streams_of[0], (IMAGES, TILES, PATCH, DV), 1.0, 6.0, ((0, 32),))
    ln_gain = jnp.clip(1.0 + 0.18 * jax.random.normal(streams_of[1], (DV,), jnp.float32), 0.1, 1.9)
    ln_bias = normal_values(streams_of[2], (DV,), 0.5, 3.0, (), jnp.float32)
    fc1_weight = normal_values(streams_of[3], (FF, DV), DV ** -0.5, 0.15625, ((0, 8),))
    fc1_bias = normal_values(streams_of[4], (FF,), 0.5, 3.0, ((0, 8),), jnp.float32)
    fc2_weight = normal_values(streams_of[5], (FF, DV), FF ** -0.5, 0.078125, ((0, 8),))
    fc2_bias = normal_values(streams_of[6], (DV,), 0.5, 3.0, (), jnp.float32)
    key_weight = normal_values(streams_of[7], (DV, KV_HEADS * HD), DV ** -0.5, 0.15625)
    value_weight = normal_values(streams_of[8], (DV, KV_HEADS * HD), DV ** -0.5, 0.15625)
    text = normal_values(streams_of[9], (TEXTS, TXT, DT), 1.0, 6.0, ((0, 16),))
    query_weight = normal_values(streams_of[10], (DT, HEADS * HD), DT ** -0.5, 0.0625, ((0, 8), (1, 2)))
    tiles = draw_tiles(jax.random.fold_in(streams_of[15], 71), 0)
    links = draw_links(jax.random.fold_in(streams_of[15], 71), 0)
    lengths = with_ends(jax.random.randint(streams_of[13], (TEXTS,), 1, TXT + 1), jax.random.fold_in(streams_of[13], 1), 1, TXT).astype(jnp.int32)
    state_grads = normal_values(streams_of[14], (IMAGES, TILES, PATCH, DV), 0.02, 0.125, ((0, 32),))
    return dict(images=images, ln_gain=ln_gain, ln_bias=ln_bias, fc1_weight=fc1_weight, fc1_bias=fc1_bias, fc2_weight=fc2_weight, fc2_bias=fc2_bias, key_weight=key_weight, value_weight=value_weight, text=text, query_weight=query_weight, tiles=tiles, links=links, lengths=lengths, state_grads=state_grads)


EPSILON = 1e-06

def normalize_layer(values, gain, shift):
    middle = lax.optimization_barrier(jnp.mean(values, axis=-1, keepdims=True))
    centered = values - middle
    spread = lax.optimization_barrier(jnp.mean(centered * centered, axis=-1, keepdims=True))
    return centered * lax.rsqrt(spread + EPSILON) * gain + shift

def normalize_heads(values):
    return values * lax.rsqrt(lax.optimization_barrier(jnp.mean(values * values, axis=-1, keepdims=True)) + EPSILON)

def gelu_slope(values):
    return 0.5 * (1.0 + lax.erf(values * 0.7071067811865476)) + values * jnp.exp(-0.5 * values * values) * 0.3989422804014327

def reference(images, ln_gain, ln_bias, fc1_weight, fc1_bias, fc2_weight, fc2_bias, key_weight, value_weight, text, query_weight, tiles, links, lengths, state_grads):
    img_rows = TILES * PATCH
    per_group = HEADS // KV_HEADS
    block_width = FF // N_ENC
    flat_rows = images.reshape(IMAGES * img_rows, DV)
    normed = normalize_layer(flat_rows.astype(jnp.float32), ln_gain, ln_bias).astype(jnp.bfloat16)
    pre = lax.dot_general(normed, fc1_weight, (((1,), (1,)), ((), ())), preferred_element_type=jnp.float32) + fc1_bias
    hidden = jax.nn.gelu(pre, approximate=False).astype(jnp.bfloat16)

    def add_block(block, total):
        start = (block * block_width).astype(jnp.int32)
        part = jnp.dot(lax.dynamic_slice_in_dim(hidden, start, block_width, 1), lax.dynamic_slice_in_dim(fc2_weight, start, block_width, 0), preferred_element_type=jnp.float32)
        rounded = lax.optimization_barrier(part.astype(jnp.bfloat16))
        return total + rounded.astype(jnp.float32)
    partial_sum = lax.fori_loop(0, N_ENC, add_block, jnp.zeros((IMAGES * img_rows, DV), jnp.float32))
    states = (flat_rows.astype(jnp.float32) + partial_sum + fc2_bias).astype(jnp.bfloat16)
    key_raw = jnp.dot(states, key_weight, preferred_element_type=jnp.float32).reshape(IMAGES * img_rows, KV_HEADS, HD)
    keys = normalize_heads(key_raw).astype(jnp.bfloat16)
    values = jnp.dot(states, value_weight, preferred_element_type=jnp.float32).astype(jnp.bfloat16).reshape(IMAGES * img_rows, KV_HEADS, HD)
    keys = keys.reshape(N_ENC, N_DEC, N_GRP, img_rows, KV_HEADS, HD).transpose(0, 2, 4, 1, 3, 5).reshape(N_ENC * N_GRP, KV_HEADS, N_DEC * img_rows, HD)
    values = values.reshape(N_ENC, N_DEC, N_GRP, img_rows, KV_HEADS, HD).transpose(0, 2, 4, 1, 3, 5).reshape(N_ENC * N_GRP, KV_HEADS, N_DEC * img_rows, HD)
    group_tiles = tiles.transpose(0, 2, 1)
    live_keys = (jnp.arange(TILES)[None, None, None, :] < group_tiles[..., None]).astype(jnp.int32)
    live_keys = jnp.broadcast_to(live_keys[..., None], (N_ENC, N_GRP, N_DEC, TILES, PATCH)).reshape(N_ENC * N_GRP, N_DEC, img_rows)
    query_raw = jnp.dot(text.reshape(TEXTS * TXT, DT), query_weight, preferred_element_type=jnp.float32).reshape(TEXTS, TXT, HEADS, HD)
    queries = normalize_heads(query_raw).astype(jnp.bfloat16).reshape(N_ENC * N_GRP, SAMP, TXT, KV_HEADS, per_group, HD)
    group_links = links.reshape(N_ENC * N_GRP, SAMP, N_DEC)
    group_lengths = lengths.reshape(N_ENC * N_GRP, SAMP)

    def attend(inputs):
        group_queries, group_keys, group_values, group_live, link_rows, length_rows = inputs
        allowed = (link_rows[:, :, None] * group_live[None, :, :]).reshape(SAMP, N_DEC * img_rows) > 0
        scores = jnp.einsum('sqghd,gkd->sghqk', group_queries.astype(jnp.float32), group_keys.astype(jnp.float32)) * HD ** (-0.5)
        weights = jnp.where(allowed[:, None, None, None, :], jnp.exp(scores), 0.0)
        probs = (weights / lax.optimization_barrier(jnp.sum(weights, axis=-1, keepdims=True))).astype(jnp.bfloat16)
        mixed = jnp.einsum('sghqk,gkd->sqghd', probs.astype(jnp.float32), group_values.astype(jnp.float32))
        valid = jnp.arange(TXT)[None, :] < length_rows[:, None]
        mixed = jnp.where(valid[:, :, None, None, None], mixed, 0.0)
        return mixed.reshape(SAMP, TXT, HEADS * HD).astype(jnp.bfloat16)
    context = lax.map(attend, (queries, keys, values, live_keys, group_links, group_lengths)).reshape(TEXTS, TXT, HEADS * HD)
    live_rows = jnp.arange(TILES)[None, :] < tiles.reshape(IMAGES)[:, None]
    live_rows = jnp.broadcast_to(live_rows[:, :, None], (IMAGES, TILES, PATCH)).reshape(IMAGES * img_rows, 1)
    cotangent = jnp.where(live_rows, state_grads.reshape(IMAGES * img_rows, DV), jnp.zeros((), state_grads.dtype))
    hidden_grad = lax.dot_general(cotangent, fc2_weight, (((1,), (1,)), ((), ())), preferred_element_type=jnp.float32)
    fc2_grad = lax.dot_general(hidden, cotangent, (((0,), (0,)), ((), ())), preferred_element_type=jnp.float32)
    pre_grad = (hidden_grad * gelu_slope(pre)).astype(jnp.bfloat16)
    fc1_grad = lax.dot_general(pre_grad, normed, (((0,), (0,)), ((), ())), preferred_element_type=jnp.float32)
    return (context, fc1_grad, fc2_grad)
```

```python
import jax
import jax.numpy as jnp
from jax import lax
from jax.sharding import PartitionSpec as P

HEADS = 32
KV_HEADS = 4
HD = 128


EPSILON = 1e-06


def normalize_layer(values, gain, shift):
    middle = jnp.mean(values, axis=-1, keepdims=True)
    centered = values - middle
    spread = jnp.mean(centered * centered, axis=-1, keepdims=True)
    return centered * lax.rsqrt(spread + EPSILON) * gain + shift


def normalize_heads(values):
    return values * lax.rsqrt(jnp.mean(values * values, axis=-1, keepdims=True) + EPSILON)


def gelu_slope(values):
    return (
        0.5 * (1.0 + lax.erf(values * 0.7071067811865476))
        + values * jnp.exp(-0.5 * values * values) * 0.3989422804014327
    )


def encoder_rows(rows, fc1_weight, fc1_bias, fc2_weight):
    pre = (
        lax.dot_general(
            rows, fc1_weight, (((1,), (1,)), ((), ())), preferred_element_type=jnp.float32
        )
        + fc1_bias
    )
    hidden = jax.nn.gelu(pre, approximate=False).astype(jnp.bfloat16)
    partial_sum = jnp.dot(hidden, fc2_weight, preferred_element_type=jnp.float32)
    return (pre, hidden, partial_sum)


def weight_terms(rows, pre, hidden, cotangent, fc2_weight):
    hidden_grad = lax.dot_general(
        cotangent, fc2_weight, (((1,), (1,)), ((), ())), preferred_element_type=jnp.float32
    )
    second_term = lax.dot_general(
        hidden, cotangent, (((0,), (0,)), ((), ())), preferred_element_type=jnp.float32
    )
    pre_grad = (hidden_grad * gelu_slope(pre)).astype(jnp.bfloat16)
    first_term = lax.dot_general(
        pre_grad, rows, (((0,), (0,)), ((), ())), preferred_element_type=jnp.float32
    )
    return (first_term, second_term)


def project_heads(states, key_columns, value_columns, heads):
    width = states.shape[-1]
    key_raw = jnp.einsum(
        "rd,dhe->hre",
        states,
        key_columns.reshape(width, heads, HD),
        preferred_element_type=jnp.float32,
    )
    keys = normalize_heads(key_raw).astype(jnp.bfloat16)
    values = jnp.einsum(
        "rd,dhe->hre",
        states,
        value_columns.reshape(width, heads, HD),
        preferred_element_type=jnp.float32,
    ).astype(jnp.bfloat16)
    return (keys, values)

def shifted(values, axis, step):
    size = lax.axis_size(axis)
    return lax.ppermute(values, axis, [(i, (i + step) % size) for i in range(size)])


def swapped(values):
    return lax.ppermute(values, "enc", [(i, i ^ 1) for i in range(lax.axis_size("enc"))])


def share_text(text_rows):
    enc_count = lax.axis_size("enc")
    rows, depth = text_rows.shape
    side = lax.axis_index("enc") % 2
    block = depth // enc_count
    parts = text_rows.reshape(rows, enc_count // 2, 2, block)
    own = lax.dynamic_index_in_dim(parts, side, 2, keepdims=False).transpose(1, 0, 2)
    away = lax.dynamic_index_in_dim(parts, 1 - side, 2, keepdims=False).transpose(1, 0, 2)
    pair = jnp.concatenate([swapped(away), own], axis=1)
    return jnp.concatenate(
        [pair] + [shifted(pair, "grp", step) for step in range(1, lax.axis_size("grp"))], axis=1
    )


def project_queries(text_blocks, weight):
    grp_count = lax.axis_size("grp")
    ring = lax.axis_size("enc") // 2
    enc_count = lax.axis_size("enc")
    place = lax.axis_index("enc") // 2
    total = None
    for step in range(ring):
        left = lax.dynamic_index_in_dim(text_blocks, (place - step) % ring, 0, keepdims=False)
        term = jnp.dot(left, weight, preferred_element_type=jnp.float32)
        total = term if total is None else total + term
        if step < ring - 1:
            weight = lax.ppermute(
                weight, "enc", [(i, (i + 2) % enc_count) for i in range(enc_count)]
            )
    columns = total.shape[1]
    total = total.reshape(grp_count, 2, -1, columns)
    arrived = swapped(total[:, 0].astype(jnp.bfloat16))
    raw = total[:, 1] + arrived.astype(jnp.float32)
    own = normalize_heads(raw.reshape(grp_count, -1, columns // HD, HD)).astype(jnp.bfloat16)
    blocks = jnp.stack(
        [own[0]] + [shifted(own[step], "grp", -step) for step in range(1, grp_count)], axis=1
    )
    start = (grp_count - lax.axis_index("grp")) % grp_count
    blocks = lax.dynamic_slice_in_dim(
        jnp.concatenate([blocks, blocks], axis=1), start, grp_count, 1
    )
    return blocks.reshape(blocks.shape[0], grp_count * columns)


def share_keys(states, key_weight, value_weight, first_head, kv_local):
    dec_count = lax.axis_size("dec")
    rows, width = states.shape
    if dec_count == 2 and kv_local * dec_count == KV_HEADS:
        keys, values = project_heads(states, key_weight, value_weight, KV_HEADS)
        paired = jnp.stack([keys, values])
        own = lax.dynamic_slice_in_dim(paired, first_head, kv_local, 1)
        away = lax.dynamic_slice_in_dim(paired, KV_HEADS - kv_local - first_head, kv_local, 1)
        arrived = shifted(away, "dec", 1)
        first = lax.axis_index("dec") == 0
        paired = jnp.stack(
            [jnp.where(first, own, arrived), jnp.where(first, arrived, own)], axis=1
        )
        return (paired[0], paired[1])
    key_columns = lax.dynamic_slice_in_dim(key_weight, first_head * HD, kv_local * HD, 1)
    value_columns = lax.dynamic_slice_in_dim(value_weight, first_head * HD, kv_local * HD, 1)
    piece = lax.all_gather(states, "dec", axis=0, tiled=True)
    key_part, value_part = project_heads(piece, key_columns, value_columns, kv_local)
    shape = (kv_local, dec_count, rows, HD)
    return (
        key_part.reshape(shape).transpose(1, 0, 2, 3),
        value_part.reshape(shape).transpose(1, 0, 2, 3),
    )


def share_grads(terms):
    dec_count = lax.axis_size("dec")
    grp_count = lax.axis_size("grp")
    rows = terms.shape[1] // (dec_count * grp_count)
    if dec_count == 2 and grp_count == 2:
        parts = terms.reshape(2, dec_count, grp_count, rows, -1)
        grp_place = lax.axis_index("grp")
        dec_place = lax.axis_index("dec")
        kept = lax.dynamic_index_in_dim(parts, grp_place, 2, keepdims=False)
        away = lax.dynamic_index_in_dim(parts, 1 - grp_place, 2, keepdims=False)
        kept = kept + shifted(away.astype(jnp.bfloat16), "grp", 1).astype(jnp.float32)
        away = lax.dynamic_index_in_dim(kept, 1 - dec_place, 1, keepdims=False)
        kept = lax.dynamic_index_in_dim(kept, dec_place, 1, keepdims=False)
        kept = kept + shifted(away.astype(jnp.bfloat16), "dec", 1).astype(jnp.float32)
        return (kept[0], kept[1])
    summed = lax.psum_scatter(
        terms.astype(jnp.bfloat16), ("dec", "grp"), scatter_dimension=1, tiled=True
    ).astype(jnp.float32)
    return (summed[0], summed[1])


def on_device(
    images,
    ln_gain,
    ln_bias,
    fc1_weight,
    fc1_bias,
    fc2_weight,
    fc2_bias,
    key_weight,
    value_weight,
    text,
    query_weight,
    tiles,
    links,
    lengths,
    state_grads,
):
    dec_count = lax.axis_size("dec")
    grp_count = lax.axis_size("grp")
    enc_place = lax.axis_index("enc")
    dec_place = lax.axis_index("dec")
    grp_place = lax.axis_index("grp")
    slots = images.shape[1]
    patch = images.shape[2]
    width = images.shape[3]
    img_rows = slots * patch
    own_rows = images.reshape(img_rows, width)
    normed = normalize_layer(own_rows.astype(jnp.float32), ln_gain, ln_bias).astype(jnp.bfloat16)
    samples = text.shape[0]
    length = text.shape[1]
    text_rows = text.reshape(samples * length, text.shape[2])
    half = query_weight.shape[1] // grp_count
    own_half = lax.dynamic_slice_in_dim(query_weight, grp_place * half, half, 1)
    own_tiles = tiles[enc_place, dec_place, grp_place]
    tile_index = jnp.arange(slots)
    own_live = jnp.broadcast_to((tile_index < own_tiles)[:, None, None], (slots, patch, 1)).reshape(
        img_rows, 1
    )
    cotangent = jnp.where(
        own_live, state_grads.reshape(img_rows, width), jnp.zeros((), state_grads.dtype)
    )
    both = lax.all_gather(jnp.stack([normed, cotangent]), "enc", axis=1, tiled=True)
    gathered, all_cotangent = both[0], both[1]
    text_blocks = share_text(text_rows)
    queries_of = project_queries(text_blocks, own_half)
    pre, hidden, partial_full = encoder_rows(gathered, fc1_weight, fc1_bias, fc2_weight)
    summed = lax.psum_scatter(
        partial_full.astype(jnp.bfloat16), "enc", scatter_dimension=0, tiled=True
    ).astype(jnp.float32)
    states = (own_rows.astype(jnp.float32) + summed + fc2_bias).astype(jnp.bfloat16)
    local_heads = query_weight.shape[1] // HD
    per_group = HEADS // KV_HEADS
    kv_local = max(1, local_heads // per_group)
    first_head = dec_place * local_heads // per_group
    keys, values = share_keys(states, key_weight, value_weight, first_head, kv_local)
    heads_each = local_heads // kv_local
    queries = queries_of
    queries = queries.reshape(samples, length, kv_local, heads_each, HD)
    dec_tiles = tiles[enc_place, :, grp_place]
    live_keys = tile_index[None, :] < dec_tiles[:, None]
    live_keys = jnp.broadcast_to(live_keys[:, :, None], (dec_count, slots, patch)).reshape(
        dec_count, img_rows
    )
    allowed = (links[:, :, None] > 0) & live_keys[None, :, :]
    scores = jnp.einsum(
        "sqghd,jgkd->sghjkq", queries, keys, preferred_element_type=jnp.float32
    ) * HD ** (-0.5)
    weights = jnp.where(allowed[:, None, None, :, :, None], jnp.exp(scores), 0.0)
    totals = jnp.sum(weights, axis=(3, 4), keepdims=True)
    probs = (weights / totals).astype(jnp.bfloat16)
    mixed = jnp.einsum("sghjkq,jgkd->sqghd", probs, values, preferred_element_type=jnp.float32)
    valid = jnp.arange(length)[None, :] < lengths[:, None]
    context = (
        jnp.where(valid[:, :, None, None, None], mixed, 0.0)
        .reshape(samples, length, local_heads * HD)
        .astype(jnp.bfloat16)
    )
    first_term, second_term = weight_terms(gathered, pre, hidden, all_cotangent, fc2_weight)
    fc1_grad, fc2_grad = share_grads(jnp.stack([first_term, second_term]))
    return (context, fc1_grad, fc2_grad)


def solution(mesh):
    in_specs = (
        P(("enc", "dec", "grp"), None, None, None),
        P(),
        P(),
        P("enc", None),
        P("enc"),
        P("enc", None),
        P(),
        P(),
        P(),
        P(("enc", "grp"), None, None),
        P("enc", "dec"),
        P(),
        P(("enc", "grp"), None),
        P(("enc", "grp")),
        P(("enc", "dec", "grp"), None, None, None),
    )
    out_specs = (
        P(("enc", "grp"), None, "dec"),
        P(("enc", "dec", "grp"), None),
        P(("enc", "dec", "grp"), None),
    )
    return jax.shard_map(
        on_device, mesh=mesh, in_specs=in_specs, out_specs=out_specs, check_vma=False
    )
```

```python
import jax
import jax.numpy as jnp
from jax import lax
from jax.sharding import PartitionSpec as P


HEADS = 32
KV_HEADS = 4
HD = 128


EPSILON = 1e-06


def normalize_layer(values, gain, shift):
    middle = jnp.mean(values, axis=-1, keepdims=True)
    centered = values - middle
    spread = jnp.mean(centered * centered, axis=-1, keepdims=True)
    return centered * lax.rsqrt(spread + EPSILON) * gain + shift


def normalize_heads(values):
    return values * lax.rsqrt(jnp.mean(values * values, axis=-1, keepdims=True) + EPSILON)


def gelu_slope(values):
    return (
        0.5 * (1.0 + lax.erf(values * 0.7071067811865476))
        + values * jnp.exp(-0.5 * values * values) * 0.3989422804014327
    )


def encoder_rows(rows, fc1_weight, fc1_bias, fc2_weight):
    pre = (
        lax.dot_general(
            rows, fc1_weight, (((1,), (1,)), ((), ())), preferred_element_type=jnp.float32
        )
        + fc1_bias
    )
    hidden = jax.nn.gelu(pre, approximate=False).astype(jnp.bfloat16)
    partial_sum = jnp.dot(hidden, fc2_weight, preferred_element_type=jnp.float32)
    return (pre, hidden, partial_sum)


def weight_terms(rows, pre, hidden, cotangent, fc2_weight):
    hidden_grad = lax.dot_general(
        cotangent, fc2_weight, (((1,), (1,)), ((), ())), preferred_element_type=jnp.float32
    )
    second_term = lax.dot_general(
        hidden, cotangent, (((0,), (0,)), ((), ())), preferred_element_type=jnp.float32
    )
    pre_grad = (hidden_grad * gelu_slope(pre)).astype(jnp.bfloat16)
    first_term = lax.dot_general(
        pre_grad, rows, (((0,), (0,)), ((), ())), preferred_element_type=jnp.float32
    )
    return (first_term, second_term)


def project_heads(states, key_columns, value_columns, heads):
    width = states.shape[-1]
    key_raw = jnp.einsum(
        "rd,dhe->hre",
        states,
        key_columns.reshape(width, heads, HD),
        preferred_element_type=jnp.float32,
    )
    keys = normalize_heads(key_raw).astype(jnp.bfloat16)
    values = jnp.einsum(
        "rd,dhe->hre",
        states,
        value_columns.reshape(width, heads, HD),
        preferred_element_type=jnp.float32,
    ).astype(jnp.bfloat16)
    return (keys, values)


def shifted(values, axis, step):
    size = lax.axis_size(axis)
    return lax.ppermute(values, axis, [(i, (i + step) % size) for i in range(size)])


def swapped(values):
    return lax.ppermute(values, "enc", [(i, i ^ 1) for i in range(lax.axis_size("enc"))])


def share_text(text_rows):
    enc_count = lax.axis_size("enc")
    _, depth = text_rows.shape
    side = lax.axis_index("enc") % 2
    block = depth // enc_count
    even = jnp.stack([text_rows[:, i * block : (i + 1) * block] for i in range(0, enc_count, 2)])
    odd = jnp.stack([text_rows[:, i * block : (i + 1) * block] for i in range(1, enc_count, 2)])
    own = jnp.where(side == 0, even, odd)
    away = jnp.where(side == 0, odd, even)
    arrived = swapped(away)
    pair = jnp.concatenate([arrived, own], axis=1)
    return jnp.concatenate(
        [pair] + [shifted(pair, "grp", step) for step in range(1, lax.axis_size("grp"))], axis=1
    )


def project_queries(text_blocks, weight, before):
    grp_count = lax.axis_size("grp")
    ring = lax.axis_size("enc") // 2
    enc_count = lax.axis_size("enc")
    place = lax.axis_index("enc") // 2
    total = None
    for step in range(ring):
        if step == max(0, ring - 2):
            weight, _ = lax.optimization_barrier((weight, before))
        left = lax.dynamic_index_in_dim(text_blocks, (place - step) % ring, 0, keepdims=False)
        term = jnp.dot(left, weight, preferred_element_type=jnp.float32)
        total = term if total is None else total + term
        if step < ring - 1:
            weight = lax.ppermute(
                weight, "enc", [(i, (i + 2) % enc_count) for i in range(enc_count)]
            )
    columns = total.shape[1]
    total = total.reshape(grp_count, 2, -1, columns)
    arrived = swapped(total[:, 0].astype(jnp.bfloat16))
    raw = total[:, 1] + arrived.astype(jnp.float32)
    own = normalize_heads(raw.reshape(grp_count, -1, columns // HD, HD)).astype(jnp.bfloat16)
    blocks = jnp.stack(
        [own[0]] + [shifted(own[step], "grp", -step) for step in range(1, grp_count)], axis=1
    )
    start = (grp_count - lax.axis_index("grp")) % grp_count
    blocks = lax.dynamic_slice_in_dim(
        jnp.concatenate([blocks, blocks], axis=1), start, grp_count, 1
    )
    return blocks.reshape(blocks.shape[0], grp_count * columns)


def share_keys(states, key_weight, value_weight, first_head, kv_local):
    dec_count = lax.axis_size("dec")
    rows, _ = states.shape
    if dec_count == 2 and kv_local * dec_count == KV_HEADS:
        keys, values = project_heads(states, key_weight, value_weight, KV_HEADS)
        paired = jnp.stack([keys, values])
        own = lax.dynamic_slice_in_dim(paired, first_head, kv_local, 1)
        away = lax.dynamic_slice_in_dim(paired, KV_HEADS - kv_local - first_head, kv_local, 1)
        arrived = shifted(away, "dec", 1)
        first = lax.axis_index("dec") == 0
        paired = jnp.stack(
            [jnp.where(first, own, arrived), jnp.where(first, arrived, own)], axis=1
        )
        return (paired[0], paired[1])
    key_columns = lax.dynamic_slice_in_dim(key_weight, first_head * HD, kv_local * HD, 1)
    value_columns = lax.dynamic_slice_in_dim(value_weight, first_head * HD, kv_local * HD, 1)
    piece = lax.all_gather(states, "dec", axis=0, tiled=True)
    key_part, value_part = project_heads(piece, key_columns, value_columns, kv_local)
    shape = (kv_local, dec_count, rows, HD)
    return (
        key_part.reshape(shape).transpose(1, 0, 2, 3),
        value_part.reshape(shape).transpose(1, 0, 2, 3),
    )


def share_grads(terms):
    dec_count = lax.axis_size("dec")
    grp_count = lax.axis_size("grp")
    rows = terms.shape[1] // (dec_count * grp_count)
    if dec_count == 2 and grp_count == 2:
        parts = terms.reshape(2, dec_count, grp_count, rows, -1)
        grp_place = lax.axis_index("grp")
        dec_place = lax.axis_index("dec")
        kept = lax.dynamic_index_in_dim(parts, grp_place, 2, keepdims=False)
        away = lax.dynamic_index_in_dim(parts, 1 - grp_place, 2, keepdims=False)
        kept = kept + shifted(away.astype(jnp.bfloat16), "grp", 1).astype(jnp.float32)
        away = lax.dynamic_index_in_dim(kept, 1 - dec_place, 1, keepdims=False)
        kept = lax.dynamic_index_in_dim(kept, dec_place, 1, keepdims=False)
        kept = kept + shifted(away.astype(jnp.bfloat16), "dec", 1).astype(jnp.float32)
        return (kept[0], kept[1])
    summed = lax.psum_scatter(
        terms.astype(jnp.bfloat16), ("dec", "grp"), scatter_dimension=1, tiled=True
    ).astype(jnp.float32)
    return (summed[0], summed[1])


def on_device(
    images,
    ln_gain,
    ln_bias,
    fc1_weight,
    fc1_bias,
    fc2_weight,
    fc2_bias,
    key_weight,
    value_weight,
    text,
    query_weight,
    tiles,
    links,
    lengths,
    state_grads,
):
    dec_count = lax.axis_size("dec")
    grp_count = lax.axis_size("grp")
    enc_place = lax.axis_index("enc")
    dec_place = lax.axis_index("dec")
    grp_place = lax.axis_index("grp")
    slots = images.shape[1]
    patch = images.shape[2]
    width = images.shape[3]
    img_rows = slots * patch
    own_rows = images.reshape(img_rows, width)
    normed = normalize_layer(own_rows.astype(jnp.float32), ln_gain, ln_bias).astype(jnp.bfloat16)
    samples = text.shape[0]
    length = text.shape[1]
    text_rows = text.reshape(samples * length, text.shape[2])
    half = query_weight.shape[1] // grp_count
    own_half = lax.dynamic_slice_in_dim(query_weight, grp_place * half, half, 1)
    own_tiles = tiles[enc_place, dec_place, grp_place]
    tile_index = jnp.arange(slots)
    own_live = jnp.broadcast_to((tile_index < own_tiles)[:, None, None], (slots, patch, 1)).reshape(
        img_rows, 1
    )
    cotangent = jnp.where(
        own_live, state_grads.reshape(img_rows, width), jnp.zeros((), state_grads.dtype)
    )
    sent = jnp.stack([normed, cotangent])
    text_rows, own_half, _ = lax.optimization_barrier((text_rows, own_half, sent))
    both = lax.all_gather(sent, "enc", axis=1, tiled=True)
    gathered, all_cotangent = both[0], both[1]
    text_blocks = share_text(text_rows)
    pre, hidden, partial_full = encoder_rows(gathered, fc1_weight, fc1_bias, fc2_weight)
    partial_full = partial_full.astype(jnp.bfloat16)
    all_cotangent, _ = lax.optimization_barrier((all_cotangent, partial_full))
    first_term, second_term = weight_terms(gathered, pre, hidden, all_cotangent, fc2_weight)
    queries_of = project_queries(text_blocks, own_half, second_term)
    summed = lax.psum_scatter(
        partial_full, "enc", scatter_dimension=0, tiled=True
    ).astype(jnp.float32)
    states = (own_rows.astype(jnp.float32) + summed + fc2_bias).astype(jnp.bfloat16)
    local_heads = query_weight.shape[1] // HD
    per_group = HEADS // KV_HEADS
    kv_local = max(1, local_heads // per_group)
    first_head = dec_place * local_heads // per_group
    keys, values = share_keys(states, key_weight, value_weight, first_head, kv_local)
    heads_each = local_heads // kv_local
    queries = queries_of
    queries = queries.reshape(samples, length, kv_local, heads_each, HD)
    dec_tiles = tiles[enc_place, :, grp_place]
    live_keys = tile_index[None, :] < dec_tiles[:, None]
    live_keys = jnp.broadcast_to(live_keys[:, :, None], (dec_count, slots, patch)).reshape(
        dec_count, img_rows
    )
    allowed = (links[:, :, None] > 0) & live_keys[None, :, :]
    scores = jnp.einsum(
        "sqghd,jgkd->sghjkq", queries, keys, preferred_element_type=jnp.float32
    ) * HD ** (-0.5)
    weights = jnp.where(allowed[:, None, None, :, :, None], jnp.exp(scores), 0.0)
    totals = jnp.sum(weights, axis=(3, 4), keepdims=True)
    probs = (weights / totals).astype(jnp.bfloat16)
    mixed = jnp.einsum("sghjkq,jgkd->sqghd", probs, values, preferred_element_type=jnp.float32)
    valid = jnp.arange(length)[None, :] < lengths[:, None]
    context = (
        jnp.where(valid[:, :, None, None, None], mixed, 0.0)
        .reshape(samples, length, local_heads * HD)
        .astype(jnp.bfloat16)
    )
    fc1_grad, fc2_grad = share_grads(jnp.stack([first_term, second_term]))
    return (context, fc1_grad, fc2_grad)


def solution(mesh):
    in_specs = (
        P(("enc", "dec", "grp"), None, None, None),
        P(),
        P(),
        P("enc", None),
        P("enc"),
        P("enc", None),
        P(),
        P(),
        P(),
        P(("enc", "grp"), None, None),
        P("enc", "dec"),
        P(),
        P(("enc", "grp"), None),
        P(("enc", "grp")),
        P(("enc", "dec", "grp"), None, None, None),
    )
    out_specs = (
        P(("enc", "grp"), None, "dec"),
        P(("enc", "dec", "grp"), None),
        P(("enc", "dec", "grp"), None),
    )
    return jax.shard_map(
        on_device, mesh=mesh, in_specs=in_specs, out_specs=out_specs, check_vma=False
    )
```
